32 devices in a mesh: fam: 4 (over y, x), owner: 8 (over z, core).
Axes of the slice: x: 2, y: 2, z: 4, core: 2. Of those that a mesh axis runs over, the one named last changes fastest.
Arguments:
- wavefunction: bfloat16 [16384, 512], P('owner'), may hold values from -6 to 6
- left_blocks: bfloat16 [4, 8, 16384, 1024], P('fam', None, 'owner'), may hold values from -0.1875 to 0.1875
- right_blocks: bfloat16 [4, 512, 512], P('fam'), may hold values from -0.0625 to 0.0625
- term_sources: int32 [4, 16, 8], replicated, may hold values from 0 to 15
- term_counts: int32 [4, 16], replicated, may hold values from 1 to 8, as said below
- sector_rows: int32 [16], replicated, may hold values from 256 to 1024
Outputs:
- sigma: bfloat16 [16384, 512], P('owner', 'fam')
The draws below stay inside these ranges and needn't reach their ends.
Inputs may be any that keep to these rules, and one draw needn't show every extreme that they name: `term_counts`: every entry lies in 1 to 8; for every output sector some family has exactly 8 live slots.
All inputs are finite; a program needn't handle non-finite values.
Results may differ from the reference program's by a relative error of at most 0.0095.
Values may be sent and summed in bfloat16 or wider, within the bound.
No kernel may reach another device: no remote copies, remote signals or barrier semaphores. Data moves between devices by JAX's collectives and lax.ppermute only.
A program may use at most 128 MiB of HBM per device.

```python
import jax
import jax.numpy as jnp
from jax import lax

S = 16
SROW = 1024
COLS = 512
KMAX = 8
FAM = 4
BOND = 16384
N_FAM = 4


def draw_term_counts(key, part):
    base = jax.random.fold_in(key, 7)
    first_key, second_key, third_key = jax.random.split(base, 3)
    first = jax.random.randint(first_key, (FAM, S), 0, KMAX)
    second = jax.random.randint(second_key, (FAM, S), 0, KMAX)
    counted = 1 + first * second // (KMAX - 1)
    busiest = jax.random.randint(third_key, (S,), 0, FAM)
    family = jnp.arange(FAM, dtype=jnp.int32)
    counted = jnp.where(family[:, None] == busiest[None, :], KMAX, counted)
    return counted.astype(jnp.int32)


def set_ends(drawn, rng, least, high):
    longest = drawn.shape.index(max(drawn.shape))
    spots = []
    for shift in (0, 1):
        where = [jax.random.randint(jax.random.fold_in(rng, axis), (), 0, length) for axis, length in enumerate(drawn.shape)]
        where[longest] = (where[longest] + shift) % drawn.shape[longest]
        spots.append(tuple(where))
    return drawn.at[spots[0]].set(least).at[spots[1]].set(high)


def levels(own_key, shape, cuts, least, largest):
    gain, own = 1.0, jax.random.fold_in(own_key, 6)
    for dim, shards_of in cuts:
        steps = jnp.exp(jax.random.uniform(jax.random.fold_in(own, dim), (shards_of,), jnp.float32, least / len(cuts), largest / len(cuts)))
        gain = gain * jnp.repeat(steps, shape[dim] // shards_of).reshape([-1 if axis == dim else 1 for axis in range(len(shape))])
    return gain


def scatter_about(key, dims, deviation, limit, shards=(), kind=jnp.bfloat16):
    array = deviation * jax.random.normal(key, dims, jnp.float32)
    if shards:
        array = array * levels(key, dims, shards, -0.22, 0.18)
    return jnp.clip(array, -limit, limit).astype(kind)


def setup_inputs(seed: int = 0) -> dict:
    key_list = jax.random.split(jax.random.key(seed), 7)
    wavefunction = scatter_about(key_list[0], (BOND, COLS), 1.0, 6.0, ((0, 8),))
    left_blocks = scatter_about(key_list[1], (FAM, KMAX, BOND, SROW), SROW ** -0.5, 0.1875, ((0, 4), (2, 8)))
    right_blocks = scatter_about(key_list[2], (FAM, COLS, COLS), (16 * COLS) ** -0.5, 0.0625, ((0, 4),))
    term_sources = set_ends(jax.random.randint(key_list[3], (FAM, S, KMAX), 0, S), jax.random.fold_in(key_list[3], 1), 0, S - 1).astype(jnp.int32)
    term_counts = draw_term_counts(jax.random.fold_in(key_list[6], 71), 0)
    sector_rows = set_ends(jax.random.randint(key_list[5], (S,), SROW // 4, SROW + 1), jax.random.fold_in(key_list[5], 1), SROW // 4, SROW).astype(jnp.int32)
    return dict(wavefunction=wavefunction, left_blocks=left_blocks, right_blocks=right_blocks, term_sources=term_sources, term_counts=term_counts, sector_rows=sector_rows)


def row_mask(sector_rows):
    rows = jnp.arange(S * SROW, dtype=jnp.int32)
    sector = rows // SROW
    return (rows % SROW) < sector_rows[sector]


def reference(wavefunction, left_blocks, right_blocks, term_sources, term_counts, sector_rows):
    keep = row_mask(sector_rows)
    masked = jnp.where(keep[:, None], wavefunction, jnp.zeros_like(wavefunction))
    stacked = masked.reshape(S, SROW, COLS)

    def one_sector(target):
        def family_step(total, family):
            def slot_step(total, slot):
                live = slot < term_counts[family, target]

                def add_term(running):
                    left = lax.dynamic_slice(left_blocks, (family, slot, target * SROW, jnp.int32(0)), (1, 1, SROW, SROW))[0, 0]
                    source = stacked[term_sources[family, target, slot]]
                    partial_value = jnp.dot(left, source, preferred_element_type=jnp.float32).astype(jnp.bfloat16)
                    return running + jnp.dot(partial_value, right_blocks[family], preferred_element_type=jnp.float32)

                def keep_same(running):
                    return running

                return lax.cond(live, add_term, keep_same, total), None

            total, _ = lax.scan(slot_step, total, jnp.arange(KMAX, dtype=jnp.int32))
            return total, None

        total, _ = lax.scan(family_step, jnp.zeros((SROW, COLS), jnp.float32), jnp.arange(N_FAM, dtype=jnp.int32))
        return total

    totals = lax.map(one_sector, jnp.arange(S, dtype=jnp.int32)).reshape(S * SROW, COLS)
    return jnp.where(keep[:, None], totals, jnp.zeros_like(totals)).astype(jnp.bfloat16)
```

```python
import functools

import jax
import jax.numpy as jnp
from jax import lax
from jax.experimental import pallas as pl
from jax.experimental.pallas import tpu as pltpu
from jax.sharding import PartitionSpec as P

SLOTS = 4
LINE = 4


def tile_of(length, most):
    tile = most
    while length % tile:
        tile //= 2
    return tile


def gather_pieces(wavefunction, fams, owners):
    rows, _ = wavefunction.shape
    fam, owner = lax.axis_index("fam"), lax.axis_index("owner")
    chips = owners // 2
    if chips > LINE:
        whole = lax.all_gather(wavefunction, "owner", axis=0, tiled=True)
        return [(whole, 0 * owner, jnp.int32(0))]
    part = rows // fams
    chip, core = owner // 2, owner % 2
    zero = jnp.int32(0)
    pieces = [(wavefunction, owner, zero)]
    swap = [(o, o ^ 1) for o in range(owners)]

    def across(value):
        return lax.ppermute(value, "owner", swap)

    pieces.append((across(wavefunction), chip * 2 + (1 - core), zero))
    mine = lax.dynamic_slice_in_dim(wavefunction, fam * part, part, 0)
    bits = [1 << i for i in range(fams.bit_length() - 1)]
    near = [d for i in range(1, chips) for d in (i, chips - i)]
    order = list(dict.fromkeys(near))
    for turn, d in enumerate(order):
        source = [(((z + d) % chips) * 2 + c, z * 2 + c) for z in range(chips) for c in range(2)]
        first = lax.ppermute(mine, "owner", source)
        held = [(first, 0)]
        for bit in bits if turn % 2 == 0 else bits[::-1]:
            pairs = [(f, f ^ bit) for f in range(fams)]
            held += [(lax.ppermute(v, "fam", pairs), m | bit) for v, m in held]
        far = (chip + d) % chips
        for value, mask in held:
            start = (fam ^ mask) * part
            pieces.append((value, far * 2 + core, start))
            pieces.append((across(value), far * 2 + (1 - core), start))
    return pieces


def kernel(sizes, sources, counts, used_rows, starts, *refs):
    pieces = refs[: sizes.pieces]
    left, right, out, whole, acc, held, ready, piece_sem, left_sem = refs[sizes.pieces :]
    fam, owner = lax.axis_index("fam"), lax.axis_index("owner")
    s = sizes
    first_row = owner * s.rows

    def sector(block):
        return (first_row + block * s.block_rows) // s.sector

    def used_out(block):
        into = lax.rem(first_row + block * s.block_rows, s.sector)
        return jnp.clip(used_rows[sector(block)] - into, 0, s.block_rows)

    def count(block):
        return counts[fam, sector(block)]

    def locate(term):
        block, slot = jnp.int32(0), term
        for b in range(s.blocks - 1):
            past = slot >= count(b)
            past = jnp.logical_and(past, block == b)
            slot = jnp.where(past, slot - count(b), slot)
            block = jnp.where(past, b + 1, block)
        return block, slot

    live = sum(count(b) for b in range(s.blocks))

    def piece_copy(i):
        height = pieces[i].shape[0]
        start = pl.multiple_of(starts[i], height)
        return pltpu.make_async_copy(
            pieces[i], whole.at[pl.ds(start, height)], piece_sem.at[i]
        )

    def tile_copy(term, tile):
        block, slot = locate(term)
        at = lax.rem(term, SLOTS)
        row = pl.multiple_of(block * s.block_rows + tile * s.tm, s.tm)
        return pltpu.make_async_copy(
            left.at[0, slot, pl.ds(row, s.tm)],
            held.at[at, pl.ds(pl.multiple_of(tile * s.tm, s.tm), s.tm)],
            left_sem.at[at, tile],
        )

    def tiles(term):
        block, _ = locate(term)
        return pl.cdiv(used_out(block), s.tm)

    def fetch(term):
        @pl.when(term < live)
        def _():
            @pl.loop(0, tiles(term))
            def _(tile):
                tile_copy(term, tile).start()

    for i in range(s.pieces):
        piece_copy(i).start()
    for term in range(SLOTS - 1):
        fetch(jnp.int32(term))

    @pl.loop(0, s.sectors)
    def _(a):
        ready[a] = 0

    for b in range(s.blocks):

        @pl.loop(0, pl.cdiv(used_out(b), s.tm))
        def _(tile):
            row = pl.multiple_of(b * s.block_rows + tile * s.tm, s.tm)
            acc[pl.ds(row, s.tm)] = jnp.zeros((s.tm, s.cols), jnp.float32)

    for i in range(s.pieces):
        piece_copy(i).wait()

    @pl.loop(0, live)
    def _(term):
        block, slot = locate(term)
        a = sources[fam, sector(block), slot]
        used = used_rows[a]
        fetch(term + SLOTS - 1)
        at = lax.rem(term, SLOTS)

        @pl.when(ready[a] == 0)
        def _():
            ready[a] = 1
            tail = pl.multiple_of(a * s.sector + (used - 1) // s.tk * s.tk, s.tk)
            rows = lax.broadcasted_iota(jnp.int32, (s.tk, s.cols), 0) + tail
            chunk = whole[pl.ds(tail, s.tk)]
            whole[pl.ds(tail, s.tk)] = jnp.where(
                rows < a * s.sector + used, chunk, jnp.zeros_like(chunk)
            )

        chunks = pl.cdiv(used, s.tk)
        base = pl.multiple_of(a * s.sector, s.sector)

        @pl.loop(0, tiles(term))
        def _(tile):
            tile_copy(term, tile).wait()
            local = pl.multiple_of(tile * s.tm, s.tm)
            row = pl.multiple_of(block * s.block_rows + tile * s.tm, s.tm)
            for n in range(1, s.sector // s.tk + 1):

                @pl.when(chunks == n)
                def _():
                    acc[pl.ds(row, s.tm)] += jnp.dot(
                        held[at, pl.ds(local, s.tm), : n * s.tk],
                        whole[pl.ds(base, n * s.tk)],
                        preferred_element_type=jnp.float32,
                    )

    width = s.cols // s.fams
    for b in range(s.blocks):

        @pl.loop(0, s.block_rows // s.tm)
        def _(tile):
            row = pl.multiple_of(b * s.block_rows + tile * s.tm, s.tm)
            rows = lax.broadcasted_iota(jnp.int32, (s.tm, s.cols), 0) + tile * s.tm
            total = jnp.where(rows < used_out(b), acc[pl.ds(row, s.tm)], 0.0)
            share = jnp.dot(
                total.astype(jnp.bfloat16), right[0], preferred_element_type=jnp.float32
            ).astype(jnp.bfloat16)
            for f in range(s.fams):
                out[f, pl.ds(row, s.tm)] = share[:, f * width : (f + 1) * width]


class Sizes:
    def __init__(self, **values):
        self.__dict__.update(values)


def body(fams, owners, wavefunction, left_blocks, right_blocks, term_sources, term_counts, sector_rows):
    rows, cols = wavefunction.shape
    slots, sector = left_blocks.shape[1], left_blocks.shape[3]
    blocks = max(rows // sector, 1)
    block_rows = rows // blocks
    found = gather_pieces(wavefunction, fams, owners)
    starts = jnp.stack([owner * rows + row for _, owner, row in found]).astype(jnp.int32)
    sizes = Sizes(
        pieces=len(found),
        fams=fams,
        rows=rows,
        cols=cols,
        sector=sector,
        sectors=sector_rows.shape[0],
        blocks=blocks,
        block_rows=block_rows,
        tm=tile_of(block_rows, 256),
        tk=tile_of(sector, 256),
    )
    hbm = pl.BlockSpec(memory_space=pltpu.MemorySpace.HBM)
    vmem = pl.BlockSpec(memory_space=pltpu.MemorySpace.VMEM)
    shares = pl.pallas_call(
        functools.partial(kernel, sizes),
        out_shape=jax.ShapeDtypeStruct((fams, rows, cols // fams), jnp.bfloat16),
        grid_spec=pltpu.PrefetchScalarGridSpec(
            num_scalar_prefetch=4,
            grid=(),
            in_specs=[hbm] * (len(found) + 1) + [vmem],
            out_specs=vmem,
            scratch_shapes=[
                pltpu.VMEM((sizes.sectors * sector, cols), jnp.bfloat16),
                pltpu.VMEM((rows, cols), jnp.float32),
                pltpu.VMEM((SLOTS, block_rows, sector), jnp.bfloat16),
                pltpu.SMEM((sizes.sectors,), jnp.int32),
                pltpu.SemaphoreType.DMA((len(found),)),
                pltpu.SemaphoreType.DMA((SLOTS, block_rows // sizes.tm)),
            ],
        ),
        compiler_params=pltpu.CompilerParams(vmem_limit_bytes=48 << 20),
        cost_estimate=pl.CostEstimate(
            flops=2 * slots * rows * sector * cols,
            bytes_accessed=2 * slots * rows * sector,
            transcendentals=0,
        ),
    )(
        term_sources,
        term_counts,
        sector_rows,
        starts,
        *[piece for piece, _, _ in found],
        left_blocks,
        right_blocks,
    )
    arrived = lax.all_to_all(shares, "fam", split_axis=0, concat_axis=0)
    return jnp.sum(arrived.astype(jnp.float32), axis=0).astype(jnp.bfloat16)


def solution(mesh):
    fams, owners = mesh.shape["fam"], mesh.shape["owner"]
    return jax.shard_map(
        functools.partial(body, fams, owners),
        mesh=mesh,
        in_specs=(
            P("owner", None),
            P("fam", None, "owner", None),
            P("fam", None, None),
            P(),
            P(),
            P(),
        ),
        out_specs=P("owner", "fam"),
        check_vma=False,
    )
```
